32 devices in a mesh: sub: 2 (over y), blk: 16 (over z, x, core).
Axes of the slice: x: 2, y: 2, z: 4, core: 2. Of those that a mesh axis runs over, the one named last changes fastest.
Arguments:
- queries: float32 [256, 1024], P('blk', 'sub'), may hold values from -0.2 to 0.2
- centroids: float32 [64, 16, 256], P('sub'), may hold values from -0.2 to 0.2
- code_ids: int32 [64, 8192], P('sub', 'blk'), may hold values from 0 to 255
- query_order: int32 [256], replicated, may hold values from 0 to 255, each once
Outputs:
- distances: float32 [256, 8192], P('sub', 'blk')
The draws below stay inside these ranges and needn't reach their ends.
Inputs may be any that keep to these rules, and one draw needn't show every extreme that they name: query_order is a permutation of the query numbers.
All inputs are finite; a program needn't handle non-finite values.
Results may differ from the reference program's by a relative error of at most 0.00039.
Values may be sent and summed in bfloat16 or wider, within the bound.
No kernel may reach another device: no remote copies, remote signals or barrier semaphores. Data moves between devices by JAX's collectives and lax.ppermute only.
A program may use at most 128 MiB of HBM per device.

```python
import jax
import jax.numpy as jnp
from jax import lax

DIM = 1024
M = 64
CENT = 256
SUBDIM = 16
QUERIES = 256
CODES = 8192


def with_ends(array, stream_key, least, largest):
    extent = array.shape
    place = [jax.random.randint(jax.random.fold_in(stream_key, axis), (), 0, extent[axis]) for axis in range(len(extent))]
    array = array.at[tuple(place)].set(least)
    longest = extent.index(max(extent))
    place[longest] = (place[longest] + 1) % extent[longest]
    return array.at[tuple(place)].set(largest)


def block_levels(own_key, extent, pieces, low, largest):
    def one(axis_at, shards_of):
        draws = jax.random.uniform(jax.random.fold_in(jax.random.fold_in(own_key, 6), axis_at), (shards_of,), jnp.float32, low / len(pieces), largest / len(pieces))
        return jnp.repeat(jnp.exp(draws), extent[axis_at] // shards_of).reshape((-1,) + (1,) * (len(extent) - axis_at - 1))

    gain = one(*pieces[0])
    for cut in pieces[1:]:
        gain = gain * one(*cut)
    return gain


def normal_values(own_key, extent, width, reach, split=(), held_as=jnp.bfloat16):
    loudness = block_levels(own_key, extent, split, -0.22, 0.18) if split else 1.0
    entries = jax.random.normal(own_key, extent, jnp.float32) * width * loudness
    return jnp.minimum(jnp.maximum(entries, -reach), reach).astype(held_as)


def setup_inputs(seed: int = 0) -> dict:
    splits = jax.random.split(jax.random.key(seed), 5)
    return {
        "queries": normal_values(splits[0], (QUERIES, DIM), 0.03125, 0.2, ((0, 16), (1, 2)), jnp.float32),
        "centroids": normal_values(splits[1], (M, SUBDIM, CENT), 0.03125, 0.2, ((0, 2),), jnp.float32),
        "code_ids": with_ends(jax.random.randint(splits[2], (M, CODES), 0, CENT), jax.random.fold_in(splits[2], 1), 0, CENT - 1).astype(jnp.int32),
        "query_order": jax.random.permutation(splits[3], QUERIES).astype(jnp.int32),
    }


def build_tables(queries, centroids):
    count = queries.shape[0]
    split_rows = queries.reshape(count, M, SUBDIM)
    total = jnp.zeros((count, M, CENT), jnp.float32)
    for column in range(SUBDIM):
        offset = split_rows[:, :, column, None] - centroids[None, :, column, :]
        total = total + offset * offset
    return total.astype(jnp.bfloat16)


def reference(queries, centroids, code_ids, query_order):
    tables = build_tables(queries, centroids)
    per_space = jnp.moveaxis(tables, 1, 0)

    def add_space(scores, items):
        space_table, space_codes = items
        picked = jnp.take(space_table.astype(jnp.float32), space_codes, axis=1)
        return scores + picked, None

    start_scores = jnp.zeros((QUERIES, CODES), jnp.float32)
    scores, _ = lax.scan(add_space, start_scores, (per_space, code_ids))
    return jnp.take(scores, query_order, axis=0)
```

```python
import jax
import jax.numpy as jnp
from jax import lax
from jax.experimental import pallas as pl
from jax.experimental.pallas import tpu as pltpu
from jax.sharding import PartitionSpec as P

LANES = 128


def decode_kernel(codes_ref, centroids_ref, high_ref, low_ref, norm_ref):
    spaces, width, centers = centroids_ref.shape
    count = codes_ref.shape[1]
    norm_ref[...] = jnp.zeros(norm_ref.shape, jnp.float32)

    def some_spaces(group, carry):
        for tile in range(count // LANES):
            lanes = pl.ds(tile * LANES, LANES)
            code_rows = codes_ref[pl.ds(pl.multiple_of(group * 8, 8), 8), lanes]
            squares = jnp.zeros((8, LANES), jnp.float32)
            for member in range(8):
                space = group * 8 + member
                codes = jnp.broadcast_to(code_rows[member : member + 1], (8, LANES))
                within = codes & (LANES - 1)
                part = codes >> (LANES.bit_length() - 1)
                pieces = []
                for row in range(0, width, 8):
                    value = None
                    for piece in range(centers // LANES):
                        table = centroids_ref[space, pl.ds(row, 8), pl.ds(piece * LANES, LANES)]
                        found = jnp.take_along_axis(table, within, axis=1)
                        value = found if piece == 0 else jnp.where(part == piece, found, value)
                    squares = squares + value * value
                    pieces.append(value)
                values = jnp.concatenate(pieces, axis=0)
                high = values.astype(jnp.bfloat16)
                rows = pl.ds(pl.multiple_of(space * width, width), width)
                high_ref[rows, lanes] = high
                low_ref[rows, lanes] = (values - high.astype(jnp.float32)).astype(jnp.bfloat16)
            norm_ref[:, lanes] += squares
        return carry

    lax.fori_loop(0, spaces // 8, some_spaces, 0)


def decode(code_ids, centroids):
    spaces, width, centers = centroids.shape
    count = code_ids.shape[1]
    return pl.pallas_call(
        decode_kernel,
        out_shape=(
            jax.ShapeDtypeStruct((spaces * width, count), jnp.bfloat16),
            jax.ShapeDtypeStruct((spaces * width, count), jnp.bfloat16),
            jax.ShapeDtypeStruct((8, count), jnp.float32),
        ),
        name="decode",
    )(code_ids, centroids)


def distance_kernel(own_rows, masks, other, order_ref, queries_ref, high_ref, low_ref, norm_ref, out_ref):
    half = lax.axis_index("sub")
    if other:
        half = 1 - half
    own = lax.axis_index("blk")
    rows = out_ref.shape[0]
    total = queries_ref.shape[0]
    order = order_ref[pl.ds(half, 1), :]
    place = lax.broadcasted_iota(jnp.int32, (total, rows), 0)
    slot = place // own_rows
    holder = jnp.full(place.shape, own, jnp.int32)
    for bit, mask in enumerate(masks):
        holder = holder ^ (((slot >> bit) & 1) * mask)
    name = holder * own_rows + place % own_rows
    pick = jnp.where(name == order, 1.0, 0.0).astype(jnp.bfloat16)
    picked = lax.dot_general(pick, queries_ref[...], (((0,), (0,)), ((), ())), preferred_element_type=jnp.float32)
    query_norm = jnp.sum(picked * picked, axis=1, keepdims=True)
    left = (picked * -2.0).astype(jnp.bfloat16)
    cross = jnp.dot(left, high_ref[...], preferred_element_type=jnp.float32)
    cross = cross + jnp.dot(left, low_ref[...], preferred_element_type=jnp.float32)
    code_norm = jnp.sum(norm_ref[...], axis=0, keepdims=True)
    out_ref[...] = cross + (query_norm + code_norm)


def distances_of(other, own_rows, masks, order, queries, high, low, norm):
    rows = order.shape[1]
    return pl.pallas_call(
        lambda *refs: distance_kernel(own_rows, masks, other, *refs),
        out_shape=jax.ShapeDtypeStruct((rows, high.shape[1]), jnp.float32),
        name="theirs" if other else "mine",
    )(order, queries, high, low, norm)


def solution(mesh):
    blocks = mesh.shape["blk"]
    halves = mesh.shape["sub"]
    masks = []
    while (1 << len(masks)) < blocks:
        masks.append(blocks >> (len(masks) + 1))

    def local(queries, centroids, code_ids, query_order):
        own_rows = queries.shape[0]
        order = query_order.reshape(halves, -1)
        rows = queries.astype(jnp.bfloat16)
        for mask in masks:
            rows = jnp.concatenate([rows, lax.ppermute(rows, "blk", [(i, i ^ mask) for i in range(blocks)])], axis=0)
        high, low, norm = decode(code_ids, centroids)
        theirs = distances_of(True, own_rows, masks, order, rows, high, low, norm)
        arrived = lax.ppermute(theirs, "sub", [(i, i ^ 1) for i in range(halves)])
        mine = distances_of(False, own_rows, masks, order, rows, high, low, norm)
        return mine + arrived

    in_specs = (P("blk", "sub"), P("sub", None, None), P("sub", "blk"), P())
    return jax.shard_map(local, mesh=mesh, in_specs=in_specs, out_specs=P("sub", "blk"), check_vma=False)
```

```python
import jax
import jax.numpy as jnp
from jax import lax
from jax.experimental import pallas as pl
from jax.experimental.pallas import tpu as pltpu
from jax.sharding import PartitionSpec as P

LANES = 128
PARTS = 2
CLOSE_BYTES = 1 << 19


def fits(array):
    return array.size * jnp.dtype(array.dtype).itemsize <= CLOSE_BYTES


def in_vmem(array):
    return pltpu.with_memory_space_constraint(array, pltpu.VMEM) if fits(array) else array


def result(shape, dtype):
    plain = jax.ShapeDtypeStruct(shape, dtype)
    return pltpu.VMEM(shape, dtype) if fits(plain) else plain


def decode_kernel(codes_ref, centroids_ref, high_ref, low_ref, norm_ref):
    spaces, width, centers = centroids_ref.shape
    count = codes_ref.shape[1]
    norm_ref[...] = jnp.zeros(norm_ref.shape, jnp.float32)

    def some_spaces(group, carry):
        for tile in range(count // LANES):
            lanes = pl.ds(tile * LANES, LANES)
            code_rows = codes_ref[pl.ds(pl.multiple_of(group * 8, 8), 8), lanes]
            squares = jnp.zeros((8, LANES), jnp.float32)
            for member in range(8):
                space = group * 8 + member
                codes = jnp.broadcast_to(code_rows[member : member + 1], (8, LANES))
                within = codes & (LANES - 1)
                part = codes >> (LANES.bit_length() - 1)
                pieces = []
                for row in range(0, width, 8):
                    value = None
                    for piece in range(centers // LANES):
                        table = centroids_ref[space, pl.ds(row, 8), pl.ds(piece * LANES, LANES)]
                        found = jnp.take_along_axis(table, within, axis=1)
                        value = found if piece == 0 else jnp.where(part == piece, found, value)
                    squares = squares + value * value
                    pieces.append(value)
                values = jnp.concatenate(pieces, axis=0)
                high = values.astype(jnp.bfloat16)
                rows = pl.ds(pl.multiple_of(space * width, width), width)
                high_ref[rows, lanes] = high
                low_ref[rows, lanes] = (values - high.astype(jnp.float32)).astype(jnp.bfloat16)
            norm_ref[:, lanes] += squares
        return carry

    lax.fori_loop(0, spaces // 8, some_spaces, 0)


def decode(part, code_ids, centroids):
    spaces, width, centers = centroids.shape
    spaces = spaces // PARTS
    count = code_ids.shape[1]
    whole = lambda *shape: pl.BlockSpec(shape, lambda i: (0,) * len(shape), memory_space=pltpu.VMEM)
    shapes = (
        result((spaces * width, count), jnp.bfloat16),
        result((spaces * width, count), jnp.bfloat16),
        result((8, count), jnp.float32),
    )
    return pl.pallas_call(
        decode_kernel,
        grid=(1,),
        in_specs=[
            pl.BlockSpec((spaces, count), lambda i: (part, 0)),
            pl.BlockSpec((spaces, width, centers), lambda i: (part, 0, 0)),
        ],
        out_specs=[whole(*shape.shape) for shape in shapes],
        out_shape=shapes,
        name="decode",
    )(code_ids, centroids)


def pick_kernel(own_rows, masks, order_ref, mine_ref, theirs_ref):
    half = lax.axis_index("sub")
    own = lax.axis_index("blk")
    place = lax.broadcasted_iota(jnp.int32, mine_ref.shape, 0)
    slot = place // own_rows
    holder = jnp.full(place.shape, own, jnp.int32)
    for bit, mask in enumerate(masks):
        holder = holder ^ (((slot >> bit) & 1) * mask)
    name = holder * own_rows + place % own_rows
    mine_ref[...] = jnp.where(name == order_ref[pl.ds(half, 1), :], 1.0, 0.0).astype(jnp.bfloat16)
    theirs_ref[...] = jnp.where(name == order_ref[pl.ds(1 - half, 1), :], 1.0, 0.0).astype(jnp.bfloat16)


def make_picks(own_rows, masks, order):
    shape = result((order.size, order.shape[1]), jnp.bfloat16)
    return pl.pallas_call(
        lambda *refs: pick_kernel(own_rows, masks, *refs),
        out_shape=(shape, shape),
        name="picks",
    )(order)


def distance_kernel(pick_ref, queries_ref, *refs):
    out_ref = refs[-1]
    picked = lax.dot_general(
        pick_ref[...], queries_ref[...], (((0,), (0,)), ((), ())), preferred_element_type=jnp.float32
    )
    total = jnp.sum(picked * picked, axis=1, keepdims=True)
    for part in range(PARTS):
        total = total + jnp.sum(refs[3 * part + 2][...], axis=0, keepdims=True)
    left = (picked * -2.0).astype(jnp.bfloat16)
    for part in range(PARTS):
        high_ref, low_ref, _ = refs[3 * part : 3 * part + 3]
        columns = high_ref.shape[0]
        piece = left[:, part * columns : (part + 1) * columns]
        total = total + jnp.dot(piece, high_ref[...], preferred_element_type=jnp.float32)
        total = total + jnp.dot(piece, low_ref[...], preferred_element_type=jnp.float32)
    out_ref[...] = total


def distances_of(pick, queries, vectors):
    return pl.pallas_call(
        distance_kernel, out_shape=result((pick.shape[1], vectors[0].shape[1]), jnp.float32)
    )(*[in_vmem(array) for array in (pick, queries, *vectors)])


def solution(mesh):
    blocks = mesh.shape["blk"]
    halves = mesh.shape["sub"]
    masks = []
    while (1 << len(masks)) < blocks:
        masks.append((blocks >> (len(masks) + 1)) | 1)

    def local(queries, centroids, code_ids, query_order):
        own_rows = queries.shape[0]
        rows = queries.astype(jnp.bfloat16)
        for mask in masks:
            arrived = lax.ppermute(rows, "blk", [(i, i ^ mask) for i in range(blocks)])
            rows = jnp.concatenate([rows, arrived], axis=0)
        pick_mine, pick_theirs = make_picks(own_rows, masks, query_order.reshape(halves, -1))
        vectors = []
        for part in range(PARTS):
            vectors.extend(decode(part, code_ids, centroids))
        theirs = distances_of(pick_theirs, rows, vectors)
        arrived = lax.ppermute(theirs, "sub", [(i, i ^ 1) for i in range(halves)])
        mine = distances_of(pick_mine, rows, vectors)
        return mine + arrived

    in_specs = (P("blk", "sub"), P("sub", None, None), P("sub", "blk"), P())
    return jax.shard_map(local, mesh=mesh, in_specs=in_specs, out_specs=P("sub", "blk"), check_vma=False)
```

```python
import jax
import jax.numpy as jnp
from jax import lax
from jax.experimental import pallas as pl
from jax.experimental.pallas import tpu as pltpu
from jax.sharding import PartitionSpec as P

LANES = 128
PARTS = 2
LEVEL = 32768.0
CLOSE_BYTES = 1 << 19


def fits(array):
    return array.size * jnp.dtype(array.dtype).itemsize <= CLOSE_BYTES


def in_vmem(array):
    return pltpu.with_memory_space_constraint(array, pltpu.VMEM) if fits(array) else array


def result(shape, dtype):
    plain = jax.ShapeDtypeStruct(shape, dtype)
    return pltpu.VMEM(shape, dtype) if fits(plain) else plain


def decode_kernel(codes_ref, centroids_ref, high_ref, low_ref, norm_ref):
    spaces, width, centers = centroids_ref.shape
    count = codes_ref.shape[1]
    norm_ref[...] = jnp.zeros(norm_ref.shape, jnp.float32)

    def some_spaces(group, carry):
        for tile in range(count // LANES):
            lanes = pl.ds(tile * LANES, LANES)
            code_rows = codes_ref[pl.ds(pl.multiple_of(group * 8, 8), 8), lanes]
            squares = jnp.zeros((8, LANES), jnp.float32)
            for member in range(8):
                space = group * 8 + member
                codes = jnp.broadcast_to(code_rows[member : member + 1], (8, LANES))
                within = codes & (LANES - 1)
                part = codes >> (LANES.bit_length() - 1)
                pieces = []
                for row in range(0, width, 8):
                    value = None
                    for piece in range(centers // LANES):
                        table = centroids_ref[space, pl.ds(row, 8), pl.ds(piece * LANES, LANES)]
                        found = jnp.take_along_axis(table, within, axis=1)
                        value = found if piece == 0 else jnp.where(part == piece, found, value)
                    squares = squares + value * value
                    pieces.append(value)
                values = jnp.concatenate(pieces, axis=0)
                high = values.astype(jnp.bfloat16)
                rows = pl.ds(pl.multiple_of(space * width, width), width)
                high_ref[rows, lanes] = high
                low_ref[rows, lanes] = (values - high.astype(jnp.float32)).astype(jnp.bfloat16)
            norm_ref[:, lanes] += squares
        return carry

    lax.fori_loop(0, spaces // 8, some_spaces, 0)


def decode(part, code_ids, centroids):
    spaces, width, centers = centroids.shape
    spaces = spaces // PARTS
    count = code_ids.shape[1]
    whole = lambda *shape: pl.BlockSpec(shape, lambda i: (0,) * len(shape), memory_space=pltpu.VMEM)
    shapes = (
        result((spaces * width, count), jnp.bfloat16),
        result((spaces * width, count), jnp.bfloat16),
        result((8, count), jnp.float32),
    )
    return pl.pallas_call(
        decode_kernel,
        grid=(1,),
        in_specs=[
            pl.BlockSpec((spaces, count), lambda i: (part, 0)),
            pl.BlockSpec((spaces, width, centers), lambda i: (part, 0, 0)),
        ],
        out_specs=[whole(*shape.shape) for shape in shapes],
        out_shape=shapes,
        name="decode",
    )(code_ids, centroids)


def pick_kernel(own_rows, masks, order_ref, mine_ref, theirs_ref):
    half = lax.axis_index("sub")
    own = lax.axis_index("blk")
    place = lax.broadcasted_iota(jnp.int32, mine_ref.shape, 0)
    slot = place // own_rows
    holder = jnp.full(place.shape, own, jnp.int32)
    for bit, mask in enumerate(masks):
        holder = holder ^ (((slot >> bit) & 1) * mask)
    name = holder * own_rows + place % own_rows
    mine_ref[...] = jnp.where(name == order_ref[pl.ds(half, 1), :], 1.0, 0.0).astype(jnp.bfloat16)
    theirs_ref[...] = jnp.where(name == order_ref[pl.ds(1 - half, 1), :], 1.0, 0.0).astype(jnp.bfloat16)


def make_picks(own_rows, masks, order):
    shape = result((order.size, order.shape[1]), jnp.bfloat16)
    return pl.pallas_call(
        lambda *refs: pick_kernel(own_rows, masks, *refs),
        out_shape=(shape, shape),
        name="picks",
    )(order)


def distance_kernel(pick_ref, queries_ref, *refs):
    vector_refs, out_refs = refs[: 3 * PARTS], refs[3 * PARTS :]
    picked = lax.dot_general(
        pick_ref[...], queries_ref[...], (((0,), (0,)), ((), ())), preferred_element_type=jnp.float32
    )
    total = jnp.sum(picked * picked, axis=1, keepdims=True)
    for part in range(PARTS):
        total = total + jnp.sum(vector_refs[3 * part + 2][...], axis=0, keepdims=True)
    left = (picked * -2.0).astype(jnp.bfloat16)
    for part in range(PARTS):
        high_ref, low_ref, _ = vector_refs[3 * part : 3 * part + 3]
        columns = high_ref.shape[0]
        piece = left[:, part * columns : (part + 1) * columns]
        total = total + jnp.dot(piece, high_ref[...], preferred_element_type=jnp.float32)
        total = total + jnp.dot(piece, low_ref[...], preferred_element_type=jnp.float32)
    if len(out_refs) == 2:
        largest = jnp.maximum(jnp.max(jnp.abs(total)), 1e-30)
        total = total * (LEVEL / largest)
        out_refs[1][...] = jnp.full(out_refs[1].shape, largest * (1.0 / LEVEL), jnp.float32)
    out_refs[0][...] = total


def distances_of(pick, queries, vectors, scaled):
    shapes = (result((pick.shape[1], vectors[0].shape[1]), jnp.float32),)
    if scaled:
        shapes += (result((8, shapes[0].shape[1]), jnp.float32),)
    return pl.pallas_call(
        distance_kernel, out_shape=shapes
    )(*[in_vmem(array) for array in (pick, queries, *vectors)])


def solution(mesh):
    blocks = mesh.shape["blk"]
    halves = mesh.shape["sub"]
    masks = []
    while (1 << len(masks)) < blocks:
        masks.append((blocks >> (len(masks) + 1)) | 1)

    def local(queries, centroids, code_ids, query_order):
        own_rows = queries.shape[0]
        rows = queries.astype(jnp.bfloat16)
        for mask in masks:
            arrived = lax.ppermute(rows, "blk", [(i, i ^ mask) for i in range(blocks)])
            rows = jnp.concatenate([rows, arrived], axis=0)
        pick_mine, pick_theirs = make_picks(own_rows, masks, query_order.reshape(halves, -1))
        vectors = []
        for part in range(PARTS):
            vectors.extend(decode(part, code_ids, centroids))
        theirs, scale = distances_of(pick_theirs, rows, vectors, True)
        swap = [(i, i ^ 1) for i in range(halves)]
        arrived = lax.ppermute(theirs.astype(jnp.float16), "sub", swap)
        scale = lax.ppermute(scale, "sub", swap)
        (mine,) = distances_of(pick_mine, rows, vectors, False)
        arrived = arrived.astype(jnp.float32).reshape(-1, *scale.shape) * scale
        return mine + arrived.reshape(mine.shape)

    in_specs = (P("blk", "sub"), P("sub", None, None), P("sub", "blk"), P())
    return jax.shard_map(local, mesh=mesh, in_specs=in_specs, out_specs=P("sub", "blk"), check_vma=False)
```

```python
import jax
import jax.numpy as jnp
from jax import lax
from jax.experimental import pallas as pl
from jax.experimental.pallas import tpu as pltpu
from jax.sharding import PartitionSpec as P

LANES = 128
PARTS = 2
SMALL = 2.0**-22
RAISE_SMALL = 2.0**37
RAISE = 2.0**8
CLOSE_BYTES = 1 << 19


def fits(array):
    return array.size * jnp.dtype(array.dtype).itemsize <= CLOSE_BYTES


def in_vmem(array):
    return pltpu.with_memory_space_constraint(array, pltpu.VMEM) if fits(array) else array


def result(shape, dtype):
    plain = jax.ShapeDtypeStruct(shape, dtype)
    return pltpu.VMEM(shape, dtype) if fits(plain) else plain


def decode_kernel(part, codes_hbm, centroids_hbm, values_ref, norm_ref, codes_ref, centroids_ref, semaphores):
    spaces, width, centers = centroids_ref.shape
    count = codes_ref.shape[1]
    first = part * spaces
    groups = spaces // 8
    copies = [pltpu.make_async_copy(codes_hbm.at[pl.ds(first, spaces)], codes_ref, semaphores.at[groups])]
    for group in range(groups):
        here = pl.ds(group * 8, 8)
        copies.append(
            pltpu.make_async_copy(
                centroids_hbm.at[pl.ds(first + group * 8, 8)], centroids_ref.at[here], semaphores.at[group]
            )
        )
    for copy in copies:
        copy.start()
    norm_ref[...] = jnp.zeros(norm_ref.shape, jnp.float32)
    copies[0].wait()

    def some_spaces(group, carry):
        here = pl.ds(pl.multiple_of(group * 8, 8), 8)
        pltpu.make_async_copy(centroids_hbm.at[here], centroids_ref.at[here], semaphores.at[group]).wait()
        for tile in range(count // LANES):
            lanes = pl.ds(tile * LANES, LANES)
            code_rows = codes_ref[here, lanes]
            squares = jnp.zeros((8, LANES), jnp.float32)
            for member in range(8):
                space = group * 8 + member
                codes = jnp.broadcast_to(code_rows[member : member + 1], (8, LANES))
                within = codes & (LANES - 1)
                part = codes >> (LANES.bit_length() - 1)
                pieces = []
                for row in range(0, width, 8):
                    value = None
                    for piece in range(centers // LANES):
                        table = centroids_ref[space, pl.ds(row, 8), pl.ds(piece * LANES, LANES)]
                        found = jnp.take_along_axis(table, within, axis=1)
                        value = found if piece == 0 else jnp.where(part == piece, found, value)
                    squares = squares + value * value
                    pieces.append(value)
                values = jnp.concatenate(pieces, axis=0)
                high = values.astype(jnp.bfloat16)
                start = pl.multiple_of(space * width, width)
                values_ref[pl.ds(start, width), lanes] = high
                rest = (values - high.astype(jnp.float32)).astype(jnp.bfloat16)
                values_ref[pl.ds(start + spaces * width, width), lanes] = rest
            norm_ref[:, lanes] += squares
        return carry

    lax.fori_loop(0, groups, some_spaces, 0)


def decode(part, code_ids, centroids):
    spaces, width, centers = centroids.shape
    spaces = spaces // PARTS
    count = code_ids.shape[1]
    return pl.pallas_call(
        lambda *refs: decode_kernel(part, *refs),
        in_specs=[pl.BlockSpec(memory_space=pl.ANY)] * 2,
        out_shape=(
            result((2 * spaces * width, count), jnp.bfloat16),
            result((8, count), jnp.float32),
        ),
        scratch_shapes=[
            pltpu.VMEM((spaces, count), jnp.int32),
            pltpu.VMEM((spaces, width, centers), jnp.float32),
            pltpu.SemaphoreType.DMA((spaces // 8 + 1,)),
        ],
        name="decode",
    )(code_ids, centroids)


def pick_kernel(own_rows, masks, order_ref, mine_ref, theirs_ref):
    half = lax.axis_index("sub")
    own = lax.axis_index("blk")
    place = lax.broadcasted_iota(jnp.int32, mine_ref.shape[::-1], 0)
    slot = place // own_rows
    holder = jnp.full(place.shape, own, jnp.int32)
    for bit, mask in enumerate(masks):
        holder = holder ^ (((slot >> bit) & 1) * mask)
    name = holder * own_rows + place % own_rows
    for pick_ref, side in ((mine_ref, half), (theirs_ref, 1 - half)):
        pick = jnp.where(name == order_ref[pl.ds(side, 1), :], -2.0, 0.0)
        pick_ref[...] = pick.T.astype(jnp.bfloat16)


def make_picks(own_rows, masks, order):
    shape = result((order.shape[1], order.size), jnp.bfloat16)
    return pl.pallas_call(
        lambda *refs: pick_kernel(own_rows, masks, *refs),
        out_shape=(shape, shape),
        name="picks",
    )(order)


def distance_kernel(send, pick_ref, queries_ref, *refs):
    left = jnp.dot(pick_ref[...], queries_ref[...], preferred_element_type=jnp.float32)
    total = 0.25 * jnp.sum(left * left, axis=1, keepdims=True)
    left = left.astype(jnp.bfloat16)
    for part in range(PARTS):
        total = total + jnp.sum(refs[2 * part + 1][...], axis=0, keepdims=True)
    for part in range(PARTS):
        columns = refs[2 * part].shape[0] // 2
        piece = left[:, part * columns : (part + 1) * columns]
        twice = jnp.concatenate([piece, piece], axis=1)
        total = total + jnp.dot(twice, refs[2 * part][...], preferred_element_type=jnp.float32)
    total = jnp.maximum(total, 0.0)
    if send:
        total = jnp.where(total < SMALL, total * -RAISE_SMALL, total * RAISE)
    refs[-1][...] = total


def distances_of(pick, queries, vectors, send):
    return pl.pallas_call(
        lambda *refs: distance_kernel(send, *refs), out_shape=result((pick.shape[0], vectors[0].shape[1]), jnp.float32)
    )(*[in_vmem(array) for array in (pick, queries, *vectors)])


def solution(mesh):
    blocks = mesh.shape["blk"]
    halves = mesh.shape["sub"]
    masks = []
    while (1 << len(masks)) < blocks:
        masks.append((blocks >> (len(masks) + 1)) | 1)

    def local(queries, centroids, code_ids, query_order):
        own_rows = queries.shape[0]
        rows = queries.astype(jnp.bfloat16)
        for mask in masks:
            arrived = lax.ppermute(rows, "blk", [(i, i ^ mask) for i in range(blocks)])
            rows = jnp.concatenate([rows, arrived], axis=0)
        pick_mine, pick_theirs = make_picks(own_rows, masks, query_order.reshape(halves, -1))
        vectors = []
        for part in range(PARTS):
            vectors.extend(decode(part, code_ids, centroids))
        theirs = distances_of(pick_theirs, rows, vectors, True)
        arrived = lax.ppermute(theirs.astype(jnp.float16), "sub", [(i, i ^ 1) for i in range(halves)])
        mine = distances_of(pick_mine, rows, vectors, False)
        arrived = arrived.astype(jnp.float32)
        return mine + arrived * jnp.where(arrived < 0.0, -1.0 / RAISE_SMALL, 1.0 / RAISE)

    in_specs = (P("blk", "sub"), P("sub", None, None), P("sub", "blk"), P())
    return jax.shard_map(local, mesh=mesh, in_specs=in_specs, out_specs=P("sub", "blk"), check_vma=False)
```

```python
import jax
import jax.numpy as jnp
from jax import lax
from jax.experimental import pallas as pl
from jax.experimental.pallas import tpu as pltpu
from jax.sharding import PartitionSpec as P

LANES = 128
PARTS = 2
SMALL = 2.0**-22
RAISE_SMALL = 2.0**37
RAISE = 2.0**8
CLOSE_BYTES = 1 << 19


def fits(array):
    return array.size * jnp.dtype(array.dtype).itemsize <= CLOSE_BYTES


def in_vmem(array):
    return pltpu.with_memory_space_constraint(array, pltpu.VMEM) if fits(array) else array


def result(shape, dtype):
    plain = jax.ShapeDtypeStruct(shape, dtype)
    return pltpu.VMEM(shape, dtype) if fits(plain) else plain


def decode_kernel(part, codes_ref, centroids_hbm, values_ref, norm_ref, centroids_ref, semaphores):
    spaces, width, centers = centroids_ref.shape
    count = codes_ref.shape[1]
    first = part * spaces
    groups = spaces // 8
    for group in range(groups):
        pltpu.make_async_copy(
            centroids_hbm.at[pl.ds(first + group * 8, 8)],
            centroids_ref.at[pl.ds(group * 8, 8)],
            semaphores.at[group],
        ).start()
    norm_ref[...] = jnp.zeros(norm_ref.shape, jnp.float32)

    def some_spaces(group, carry):
        here = pl.ds(pl.multiple_of(group * 8, 8), 8)
        pltpu.make_async_copy(centroids_hbm.at[here], centroids_ref.at[here], semaphores.at[group]).wait()
        for tile in range(count // LANES):
            lanes = pl.ds(tile * LANES, LANES)
            code_rows = codes_ref[pl.ds(pl.multiple_of(first + group * 8, 8), 8), lanes]
            squares = jnp.zeros((8, LANES), jnp.float32)
            for member in range(8):
                space = group * 8 + member
                codes = jnp.broadcast_to(code_rows[member : member + 1], (8, LANES))
                within = codes & (LANES - 1)
                part = codes >> (LANES.bit_length() - 1)
                pieces = []
                for row in range(0, width, 8):
                    value = None
                    for piece in range(centers // LANES):
                        table = centroids_ref[space, pl.ds(row, 8), pl.ds(piece * LANES, LANES)]
                        found = jnp.take_along_axis(table, within, axis=1)
                        value = found if piece == 0 else jnp.where(part == piece, found, value)
                    squares = squares + value * value
                    pieces.append(value)
                values = jnp.concatenate(pieces, axis=0)
                high = values.astype(jnp.bfloat16)
                start = pl.multiple_of(space * width, width)
                values_ref[pl.ds(start, width), lanes] = high
                rest = (values - high.astype(jnp.float32)).astype(jnp.bfloat16)
                values_ref[pl.ds(start + spaces * width, width), lanes] = rest
            norm_ref[:, lanes] += squares
        return carry

    lax.fori_loop(0, groups, some_spaces, 0)


def decode(part, code_ids, centroids):
    spaces, width, centers = centroids.shape
    spaces = spaces // PARTS
    count = code_ids.shape[1]
    return pl.pallas_call(
        lambda *refs: decode_kernel(part, *refs),
        in_specs=[pl.BlockSpec(memory_space=pltpu.VMEM), pl.BlockSpec(memory_space=pl.ANY)],
        out_shape=(
            result((2 * spaces * width, count), jnp.bfloat16),
            result((8, count), jnp.float32),
        ),
        scratch_shapes=[
            pltpu.VMEM((spaces, width, centers), jnp.float32),
            pltpu.SemaphoreType.DMA((spaces // 8,)),
        ],
        name="decode",
    )(in_vmem(code_ids), centroids)


def pick_kernel(own_rows, masks, order_ref, mine_ref, theirs_ref):
    half = lax.axis_index("sub")
    own = lax.axis_index("blk")
    place = lax.broadcasted_iota(jnp.int32, mine_ref.shape[::-1], 0)
    slot = place // own_rows
    holder = jnp.full(place.shape, own, jnp.int32)
    for bit, mask in enumerate(masks):
        holder = holder ^ (((slot >> bit) & 1) * mask)
    name = holder * own_rows + place % own_rows
    for pick_ref, side in ((mine_ref, half), (theirs_ref, 1 - half)):
        pick = jnp.where(name == order_ref[pl.ds(side, 1), :], -2.0, 0.0)
        pick_ref[...] = pick.T.astype(jnp.bfloat16)


def make_picks(own_rows, masks, order):
    shape = result((order.shape[1], order.size), jnp.bfloat16)
    return pl.pallas_call(
        lambda *refs: pick_kernel(own_rows, masks, *refs),
        out_shape=(shape, shape),
        name="picks",
    )(order)


def distance_kernel(send, pick_ref, queries_ref, *refs):
    left = jnp.dot(pick_ref[...], queries_ref[...], preferred_element_type=jnp.float32)
    total = 0.25 * jnp.sum(left * left, axis=1, keepdims=True)
    left = left.astype(jnp.bfloat16)
    for part in range(PARTS):
        total = total + jnp.sum(refs[2 * part + 1][...], axis=0, keepdims=True)
    for part in range(PARTS):
        columns = refs[2 * part].shape[0] // 2
        piece = left[:, part * columns : (part + 1) * columns]
        twice = jnp.concatenate([piece, piece], axis=1)
        total = total + jnp.dot(twice, refs[2 * part][...], preferred_element_type=jnp.float32)
    total = jnp.maximum(total, 0.0)
    if send:
        total = jnp.where(total < SMALL, total * -RAISE_SMALL, total * RAISE)
    refs[-1][...] = total


def distances_of(pick, queries, vectors, send):
    return pl.pallas_call(
        lambda *refs: distance_kernel(send, *refs),
        out_shape=result((pick.shape[0], vectors[0].shape[1]), jnp.float32),
    )(*[in_vmem(array) for array in (pick, queries, *vectors)])


def solution(mesh):
    blocks = mesh.shape["blk"]
    halves = mesh.shape["sub"]
    masks = []
    while (1 << len(masks)) < blocks:
        masks.append((blocks >> (len(masks) + 1)) | 1)

    def local(queries, centroids, code_ids, query_order):
        own_rows = queries.shape[0]
        mate = [(i, i ^ 1) for i in range(blocks)]
        code_ids = lax.ppermute(code_ids, "blk", mate)
        rows = queries.astype(jnp.bfloat16)
        for mask in masks:
            arrived = lax.ppermute(rows, "blk", [(i, i ^ mask) for i in range(blocks)])
            rows = jnp.concatenate([rows, arrived], axis=0)
        pick_mine, pick_theirs = make_picks(own_rows, masks, query_order.reshape(halves, -1))
        vectors = []
        for part in range(PARTS):
            vectors.extend(decode(part, code_ids, centroids))
        theirs = distances_of(pick_theirs, rows, vectors, True)
        across = [(i, (i ^ 1) ^ blocks) for i in range(halves * blocks)]
        arrived = lax.ppermute(theirs.astype(jnp.float16), ("sub", "blk"), across)
        mine = distances_of(pick_mine, rows, vectors, False)
        mine = lax.ppermute(mine, "blk", mate)
        arrived = arrived.astype(jnp.float32)
        return mine + arrived * jnp.where(arrived < 0.0, -1.0 / RAISE_SMALL, 1.0 / RAISE)

    in_specs = (P("blk", "sub"), P("sub", None, None), P("sub", "blk"), P())
    return jax.shard_map(local, mesh=mesh, in_specs=in_specs, out_specs=P("sub", "blk"), check_vma=False)
```

```python
import jax
import jax.numpy as jnp
from jax import lax
from jax.experimental import pallas as pl
from jax.experimental.pallas import tpu as pltpu
from jax.sharding import PartitionSpec as P

LANES = 128
PARTS = 2
SMALL = 2.0**-22
RAISE_SMALL = 2.0**37
RAISE = 2.0**8
STRETCH = 163840.0
CLOSE_BYTES = 1 << 19


def fits(array):
    return array.size * jnp.dtype(array.dtype).itemsize <= CLOSE_BYTES


def in_vmem(array):
    return pltpu.with_memory_space_constraint(array, pltpu.VMEM) if fits(array) else array


def result(shape, dtype):
    plain = jax.ShapeDtypeStruct(shape, dtype)
    return pltpu.VMEM(shape, dtype) if fits(plain) else plain


def decode_kernel(part, codes_ref, centroids_hbm, values_ref, norm_ref, centroids_ref, semaphores):
    spaces, width, centers = centroids_ref.shape
    count = codes_ref.shape[1]
    first = part * spaces
    groups = spaces // 8
    for group in range(groups):
        pltpu.make_async_copy(
            centroids_hbm.at[pl.ds(first + group * 8, 8)],
            centroids_ref.at[pl.ds(group * 8, 8)],
            semaphores.at[group],
        ).start()
    norm_ref[...] = jnp.zeros(norm_ref.shape, jnp.float32)

    def some_spaces(group, carry):
        here = pl.ds(pl.multiple_of(group * 8, 8), 8)
        pltpu.make_async_copy(centroids_hbm.at[here], centroids_ref.at[here], semaphores.at[group]).wait()
        for tile in range(count // LANES):
            lanes = pl.ds(tile * LANES, LANES)
            code_rows = codes_ref[pl.ds(pl.multiple_of(first + group * 8, 8), 8), lanes]
            squares = jnp.zeros((8, LANES), jnp.float32)
            for member in range(8):
                space = group * 8 + member
                codes = jnp.broadcast_to(code_rows[member : member + 1], (8, LANES))
                within = codes & (LANES - 1)
                part = codes >> (LANES.bit_length() - 1)
                pieces = []
                for row in range(0, width, 8):
                    value = None
                    for piece in range(centers // LANES):
                        table = centroids_ref[space, pl.ds(row, 8), pl.ds(piece * LANES, LANES)]
                        found = jnp.take_along_axis(table, within, axis=1)
                        value = found if piece == 0 else jnp.where(part == piece, found, value)
                    squares = squares + value * value
                    pieces.append(value)
                values = jnp.concatenate(pieces, axis=0)
                high = values.astype(jnp.bfloat16)
                start = pl.multiple_of(space * width, width)
                values_ref[pl.ds(start, width), lanes] = high
                rest = (values - high.astype(jnp.float32)).astype(jnp.bfloat16)
                values_ref[pl.ds(start + spaces * width, width), lanes] = rest
            norm_ref[:, lanes] += squares
        return carry

    lax.fori_loop(0, groups, some_spaces, 0)


def decode(part, code_ids, centroids):
    spaces, width, centers = centroids.shape
    spaces = spaces // PARTS
    count = code_ids.shape[1]
    return pl.pallas_call(
        lambda *refs: decode_kernel(part, *refs),
        in_specs=[pl.BlockSpec(memory_space=pltpu.VMEM), pl.BlockSpec(memory_space=pl.ANY)],
        out_shape=(
            result((2 * spaces * width, count), jnp.bfloat16),
            result((8, count), jnp.float32),
        ),
        scratch_shapes=[
            pltpu.VMEM((spaces, width, centers), jnp.float32),
            pltpu.SemaphoreType.DMA((spaces // 8,)),
        ],
        name="decode",
    )(in_vmem(code_ids), centroids)


def pick_kernel(own_rows, masks, order_ref, mine_ref, theirs_ref):
    half = lax.axis_index("sub")
    own = lax.axis_index("blk")
    place = lax.broadcasted_iota(jnp.int32, mine_ref.shape[::-1], 0)
    slot = place // own_rows
    holder = jnp.full(place.shape, own, jnp.int32)
    for bit, mask in enumerate(masks):
        holder = holder ^ (((slot >> bit) & 1) * mask)
    name = holder * own_rows + place % own_rows
    for pick_ref, side in ((mine_ref, half), (theirs_ref, 1 - half)):
        pick = jnp.where(name == order_ref[pl.ds(side, 1), :], 1.0, 0.0)
        pick_ref[...] = pick.T.astype(jnp.bfloat16)


def make_picks(own_rows, masks, order):
    shape = result((order.shape[1], order.size), jnp.bfloat16)
    return pl.pallas_call(
        lambda *refs: pick_kernel(own_rows, masks, *refs),
        out_shape=(shape, shape),
        name="picks",
    )(order)


def picked(pick_ref, *row_refs):
    total, first = None, 0
    for row_ref in row_refs:
        columns = pick_ref[:, pl.ds(first, row_ref.shape[0])]
        rows = jnp.dot(columns, row_ref[...], preferred_element_type=jnp.float32)
        total, first = rows if total is None else total + rows, first + row_ref.shape[0]
    return total


def distance_kernel(send, pick_ref, high_ref, low_ref, mate_high_ref, mate_low_ref, *refs):
    high = picked(pick_ref, high_ref, mate_high_ref)
    low = picked(pick_ref, low_ref, mate_low_ref)
    whole = high + low
    rows = whole.shape[0]
    both = jnp.concatenate([high, low], axis=0).astype(jnp.bfloat16)
    cross = jnp.zeros((rows, refs[-1].shape[1]), jnp.float32)
    total = (1.0 / STRETCH**2) * jnp.sum(whole * whole, axis=1, keepdims=True)
    for part in range(PARTS):
        total = total + jnp.sum(refs[2 * part + 1][...], axis=0, keepdims=True)
    for part in range(PARTS):
        columns = refs[2 * part].shape[0] // 2
        piece = both[:, part * columns : (part + 1) * columns]
        product = jnp.dot(piece, refs[2 * part][:columns], preferred_element_type=jnp.float32)
        cross = cross + (product[:rows] + product[rows:])
        cross = cross + jnp.dot(piece[:rows], refs[2 * part][columns:], preferred_element_type=jnp.float32)
    total = jnp.maximum(total - (2.0 / STRETCH) * cross, 0.0)
    if send:
        total = jnp.where(total < SMALL, total * -RAISE_SMALL, total * RAISE)
    refs[-1][...] = total


def distances_of(pick, queries, vectors, send):
    return pl.pallas_call(
        lambda *refs: distance_kernel(send, *refs),
        out_shape=result((pick.shape[0], vectors[0].shape[1]), jnp.float32),
    )(*[in_vmem(array) for array in (pick, *queries, *vectors)])


def split(rows):
    rows = rows.astype(jnp.float32)
    high = lax.reduce_precision(rows, 8, 7)
    return high.astype(jnp.bfloat16), (rows - high).astype(jnp.bfloat16)


def solution(mesh):
    blocks = mesh.shape["blk"]
    halves = mesh.shape["sub"]
    masks = []
    while (1 << len(masks)) < blocks:
        masks.append((blocks >> (len(masks) + 1)) | 1)

    def local(queries, centroids, code_ids, query_order):
        own_rows = queries.shape[0]
        mate = [(i, i ^ 1) for i in range(blocks)]
        code_ids = lax.ppermute(code_ids, "blk", mate)
        rows = (queries * STRETCH).astype(jnp.float16)
        for step, mask in enumerate(masks):
            arrived = lax.ppermute(rows, "blk", [(i, i ^ mask) for i in range(blocks)])
            if step + 1 < len(masks):
                rows = jnp.concatenate([rows, arrived], axis=0)
            else:
                queries = (*split(rows), *split(arrived))
        pick_mine, pick_theirs = make_picks(own_rows, masks, query_order.reshape(halves, -1))
        vectors = []
        for part in range(PARTS):
            vectors.extend(decode(part, code_ids, centroids))
        theirs = distances_of(pick_theirs, queries, vectors, True)
        across = [(i, (i ^ 1) ^ blocks) for i in range(halves * blocks)]
        arrived = lax.ppermute(theirs.astype(jnp.float16), ("sub", "blk"), across)
        mine = distances_of(pick_mine, queries, vectors, False)
        mine = lax.ppermute(mine, "blk", mate)
        arrived = arrived.astype(jnp.float32)
        return mine + arrived * jnp.where(arrived < 0.0, -1.0 / RAISE_SMALL, 1.0 / RAISE)

    in_specs = (P("blk", "sub"), P("sub", None, None), P("sub", "blk"), P())
    return jax.shard_map(local, mesh=mesh, in_specs=in_specs, out_specs=P("sub", "blk"), check_vma=False)
```

```python
import jax
import jax.numpy as jnp
from jax import lax
from jax.experimental import pallas as pl
from jax.experimental.pallas import tpu as pltpu
from jax.sharding import PartitionSpec as P

LANES = 128
PARTS = 2
SMALL = 2.0**-22
RAISE_SMALL = 2.0**37
RAISE = 2.0**8
STRETCH = 2.0**17
CLOSE_BYTES = 1 << 19


def fits(array):
    return array.size * jnp.dtype(array.dtype).itemsize <= CLOSE_BYTES


def in_vmem(array):
    return pltpu.with_memory_space_constraint(array, pltpu.VMEM) if fits(array) else array


def result(shape, dtype):
    plain = jax.ShapeDtypeStruct(shape, dtype)
    return pltpu.VMEM(shape, dtype) if fits(plain) else plain


def decode_kernel(part, codes_ref, centroids_hbm, values_ref, norm_ref, centroids_ref, semaphores):
    spaces, width, centers = centroids_ref.shape
    count = codes_ref.shape[1]
    first = part * spaces
    groups = spaces // 8
    for group in range(groups):
        pltpu.make_async_copy(
            centroids_hbm.at[pl.ds(first + group * 8, 8)],
            centroids_ref.at[pl.ds(group * 8, 8)],
            semaphores.at[group],
        ).start()
    norm_ref[...] = jnp.zeros(norm_ref.shape, jnp.float32)

    def some_spaces(group, carry):
        here = pl.ds(pl.multiple_of(group * 8, 8), 8)
        pltpu.make_async_copy(centroids_hbm.at[here], centroids_ref.at[here], semaphores.at[group]).wait()
        for tile in range(count // LANES):
            lanes = pl.ds(tile * LANES, LANES)
            code_rows = codes_ref[pl.ds(pl.multiple_of(first + group * 8, 8), 8), lanes]
            squares = jnp.zeros((8, LANES), jnp.float32)
            for member in range(8):
                space = group * 8 + member
                codes = jnp.broadcast_to(code_rows[member : member + 1], (8, LANES))
                within = codes & (LANES - 1)
                part = codes >> (LANES.bit_length() - 1)
                pieces = []
                for row in range(0, width, 8):
                    value = None
                    for piece in range(centers // LANES):
                        table = centroids_ref[space, pl.ds(row, 8), pl.ds(piece * LANES, LANES)]
                        found = jnp.take_along_axis(table, within, axis=1)
                        value = found if piece == 0 else jnp.where(part == piece, found, value)
                    squares = squares + value * value
                    pieces.append(value)
                values = jnp.concatenate(pieces, axis=0)
                high = values.astype(jnp.bfloat16)
                start = pl.multiple_of(space * width, width)
                values_ref[pl.ds(start, width), lanes] = high
                rest = (values - high.astype(jnp.float32)).astype(jnp.bfloat16)
                values_ref[pl.ds(start + spaces * width, width), lanes] = rest
            norm_ref[:, lanes] += squares
        return carry

    lax.fori_loop(0, groups, some_spaces, 0)


def decode(part, code_ids, centroids):
    spaces, width, centers = centroids.shape
    spaces = spaces // PARTS
    count = code_ids.shape[1]
    return pl.pallas_call(
        lambda *refs: decode_kernel(part, *refs),
        in_specs=[pl.BlockSpec(memory_space=pltpu.VMEM), pl.BlockSpec(memory_space=pl.ANY)],
        out_shape=(
            result((2 * spaces * width, count), jnp.bfloat16),
            result((8, count), jnp.float32),
        ),
        scratch_shapes=[
            pltpu.VMEM((spaces, width, centers), jnp.float32),
            pltpu.SemaphoreType.DMA((spaces // 8,)),
        ],
        name="decode",
    )(in_vmem(code_ids), centroids)


def pick_kernel(own_rows, masks, order_ref, mine_ref, theirs_ref):
    half = lax.axis_index("sub")
    own = lax.axis_index("blk")
    place = lax.broadcasted_iota(jnp.int32, mine_ref.shape[::-1], 0)
    slot = place // own_rows
    holder = jnp.full(place.shape, own, jnp.int32)
    for bit, mask in enumerate(masks):
        holder = holder ^ (((slot >> bit) & 1) * mask)
    name = holder * own_rows + place % own_rows
    for pick_ref, side in ((mine_ref, half), (theirs_ref, 1 - half)):
        pick = jnp.where(name == order_ref[pl.ds(side, 1), :], 1.0, 0.0)
        pick_ref[...] = pick.T.astype(jnp.bfloat16)


def make_picks(own_rows, masks, order):
    shape = result((order.shape[1], order.size), jnp.bfloat16)
    return pl.pallas_call(
        lambda *refs: pick_kernel(own_rows, masks, *refs),
        out_shape=(shape, shape),
        name="picks",
    )(order)


def picked(pick_ref, *row_refs):
    total, first = None, 0
    for row_ref in row_refs:
        columns = pick_ref[:, pl.ds(first, row_ref.shape[0])]
        rows = jnp.dot(columns, row_ref[...], preferred_element_type=jnp.float32)
        total, first = rows if total is None else total + rows, first + row_ref.shape[0]
    return total


def distance_kernel(send, pick_ref, high_ref, low_ref, mate_high_ref, mate_low_ref, *refs):
    high = picked(pick_ref, high_ref, mate_high_ref)
    low = picked(pick_ref, low_ref, mate_low_ref)
    whole = high + low
    rows = whole.shape[0]
    both = jnp.concatenate([high, low], axis=0).astype(jnp.bfloat16)
    cross = jnp.zeros((rows, refs[-1].shape[1]), jnp.float32)
    total = (1.0 / STRETCH**2) * jnp.sum(whole * whole, axis=1, keepdims=True)
    for part in range(PARTS):
        total = total + jnp.sum(refs[2 * part + 1][...], axis=0, keepdims=True)
    for part in range(PARTS):
        columns = refs[2 * part].shape[0] // 2
        piece = both[:, part * columns : (part + 1) * columns]
        product = jnp.dot(piece, refs[2 * part][:columns], preferred_element_type=jnp.float32)
        cross = cross + (product[:rows] + product[rows:])
        cross = cross + jnp.dot(piece[:rows], refs[2 * part][columns:], preferred_element_type=jnp.float32)
    total = jnp.maximum(total - (2.0 / STRETCH) * cross, 0.0)
    if send:
        total = jnp.where(total < SMALL, total * -RAISE_SMALL, total * RAISE)
    refs[-1][...] = total


def distances_of(pick, queries, vectors, send):
    return pl.pallas_call(
        lambda *refs: distance_kernel(send, *refs), out_shape=result((pick.shape[0], vectors[0].shape[1]), jnp.float32)
    )(*[in_vmem(array) for array in (pick, *queries, *vectors)])


def round_queries(queries):
    place = lax.broadcasted_iota(jnp.int32, queries.shape, 0) * queries.shape[1]
    place = (place + lax.broadcasted_iota(jnp.int32, queries.shape, 1)).astype(jnp.float32) * 0.618034
    offset = (place - jnp.floor(place)) * 2.0 - 1.0
    stretched = queries * STRETCH
    step = jnp.exp2(jnp.floor(jnp.log2(jnp.maximum(jnp.abs(stretched), 2.0**-14))) - 11.0)
    return (stretched + offset * step).astype(jnp.float16)


def split(rows):
    rows = rows.astype(jnp.float32)
    high = lax.reduce_precision(rows, 8, 7)
    return high.astype(jnp.bfloat16), (rows - high).astype(jnp.bfloat16)


def solution(mesh):
    blocks = mesh.shape["blk"]
    halves = mesh.shape["sub"]
    masks = []
    while (1 << len(masks)) < blocks:
        masks.append((blocks >> (len(masks) + 1)) | 1)

    def local(queries, centroids, code_ids, query_order):
        own_rows = queries.shape[0]
        mate = [(i, i ^ 1) for i in range(blocks)]
        code_ids = lax.ppermute(code_ids, "blk", mate)
        rows = round_queries(queries)
        for step, mask in enumerate(masks):
            arrived = lax.ppermute(rows, "blk", [(i, i ^ mask) for i in range(blocks)])
            if step + 1 < len(masks):
                rows = jnp.concatenate([rows, arrived], axis=0)
            else:
                queries = (*split(rows), *split(arrived))
        pick_mine, pick_theirs = make_picks(own_rows, masks, query_order.reshape(halves, -1))
        vectors = []
        for part in range(PARTS):
            vectors.extend(decode(part, code_ids, centroids))
        theirs = distances_of(pick_theirs, queries, vectors, True)
        across = [(i, (i ^ 1) ^ blocks) for i in range(halves * blocks)]
        arrived = lax.ppermute(theirs.astype(jnp.float16), ("sub", "blk"), across)
        mine = distances_of(pick_mine, queries, vectors, False)
        mine = lax.ppermute(mine, "blk", mate)
        arrived = arrived.astype(jnp.float32)
        return mine + arrived * jnp.where(arrived < 0.0, -1.0 / RAISE_SMALL, 1.0 / RAISE)

    in_specs = (P("blk", "sub"), P("sub", None, None), P("sub", "blk"), P())
    return jax.shard_map(local, mesh=mesh, in_specs=in_specs, out_specs=P("sub", "blk"), check_vma=False)
```

```python
import jax
import jax.numpy as jnp
from jax import lax
from jax.experimental import pallas as pl
from jax.experimental.pallas import tpu as pltpu
from jax.sharding import PartitionSpec as P

LANES = 128
PARTS = 2
SMALL = 2.0**-22
RAISE_SMALL = 2.0**37
RAISE = 2.0**8
STRETCH = 2.0**17
CLOSE_BYTES = 1 << 19


def fits(array):
    return array.size * jnp.dtype(array.dtype).itemsize <= CLOSE_BYTES


def in_vmem(array):
    return pltpu.with_memory_space_constraint(array, pltpu.VMEM) if fits(array) else array


def result(shape, dtype):
    plain = jax.ShapeDtypeStruct(shape, dtype)
    return pltpu.VMEM(shape, dtype) if fits(plain) else plain


def decode_kernel(part, codes_ref, centroids_hbm, values_ref, norm_ref, centroids_ref, semaphores):
    spaces, width, centers = centroids_ref.shape
    count = codes_ref.shape[1]
    first = part * spaces
    groups = spaces // 8
    for group in range(groups):
        pltpu.make_async_copy(
            centroids_hbm.at[pl.ds(first + group * 8, 8)],
            centroids_ref.at[pl.ds(group * 8, 8)],
            semaphores.at[group],
        ).start()
    norm_ref[...] = jnp.zeros(norm_ref.shape, jnp.float32)

    def some_spaces(group, carry):
        here = pl.ds(pl.multiple_of(group * 8, 8), 8)
        pltpu.make_async_copy(centroids_hbm.at[here], centroids_ref.at[here], semaphores.at[group]).wait()
        for tile in range(count // LANES):
            lanes = pl.ds(tile * LANES, LANES)
            code_rows = codes_ref[pl.ds(pl.multiple_of(first + group * 8, 8), 8), lanes]
            squares = jnp.zeros((8, LANES), jnp.float32)
            for member in range(8):
                space = group * 8 + member
                codes = jnp.broadcast_to(code_rows[member : member + 1], (8, LANES))
                within = codes & (LANES - 1)
                part = codes >> (LANES.bit_length() - 1)
                pieces = []
                for row in range(0, width, 8):
                    value = None
                    for piece in range(centers // LANES):
                        table = centroids_ref[space, pl.ds(row, 8), pl.ds(piece * LANES, LANES)]
                        found = jnp.take_along_axis(table, within, axis=1)
                        value = found if piece == 0 else jnp.where(part == piece, found, value)
                    squares = squares + value * value
                    pieces.append(value)
                values = jnp.concatenate(pieces, axis=0)
                high = values.astype(jnp.bfloat16)
                start = pl.multiple_of(space * width, width)
                values_ref[pl.ds(start, width), lanes] = high
                rest = (values - high.astype(jnp.float32)).astype(jnp.bfloat16)
                values_ref[pl.ds(start + spaces * width, width), lanes] = rest
            norm_ref[:, lanes] += squares
        return carry

    lax.fori_loop(0, groups, some_spaces, 0)


def decode(part, code_ids, centroids):
    spaces, width, centers = centroids.shape
    spaces = spaces // PARTS
    count = code_ids.shape[1]
    return pl.pallas_call(
        lambda *refs: decode_kernel(part, *refs),
        in_specs=[pl.BlockSpec(memory_space=pltpu.VMEM), pl.BlockSpec(memory_space=pl.ANY)],
        out_shape=(
            result((2 * spaces * width, count), jnp.bfloat16),
            result((8, count), jnp.float32),
        ),
        scratch_shapes=[
            pltpu.VMEM((spaces, width, centers), jnp.float32),
            pltpu.SemaphoreType.DMA((spaces // 8,)),
        ],
        name="decode",
    )(in_vmem(code_ids), centroids)


def pick_kernel(own_rows, masks, order_ref, mine_ref, theirs_ref):
    half = lax.axis_index("sub")
    own = lax.axis_index("blk")
    place = lax.broadcasted_iota(jnp.int32, mine_ref.shape[::-1], 0)
    slot = place // own_rows
    holder = jnp.full(place.shape, own, jnp.int32)
    for bit, mask in enumerate(masks):
        holder = holder ^ (((slot >> bit) & 1) * mask)
    name = holder * own_rows + place % own_rows
    for pick_ref, side in ((mine_ref, half), (theirs_ref, 1 - half)):
        pick = jnp.where(name == order_ref[pl.ds(side, 1), :], 1.0, 0.0)
        pick_ref[...] = pick.T.astype(jnp.bfloat16)


def make_picks(own_rows, masks, order):
    shape = result((order.shape[1], order.size), jnp.bfloat16)
    return pl.pallas_call(
        lambda *refs: pick_kernel(own_rows, masks, *refs),
        out_shape=(shape, shape),
        name="picks",
    )(in_vmem(order))


def early_kernel(theirs_ref, mine_ref, high_ref, low_ref, *out_refs):
    for side, pick_ref in enumerate((theirs_ref, mine_ref)):
        pick = pick_ref[:, : high_ref.shape[0]]
        for part, row_ref in enumerate((high_ref, low_ref)):
            rows = jnp.dot(pick, row_ref[...], preferred_element_type=jnp.float32)
            out_refs[2 * side + part][...] = rows.astype(jnp.bfloat16)


def pick_early(pick_theirs, pick_mine, high, low):
    shape = result((pick_mine.shape[0], high.shape[1]), jnp.bfloat16)
    return pl.pallas_call(early_kernel, out_shape=(shape,) * 4, name="early")(
        *[in_vmem(array) for array in (pick_theirs, pick_mine, high, low)]
    )


def distance_kernel(send, pick_ref, high_ref, low_ref, mate_high_ref, mate_low_ref, *refs):
    pick = pick_ref[:, pick_ref.shape[1] - mate_high_ref.shape[0] :]
    high = jnp.dot(pick, mate_high_ref[...], preferred_element_type=jnp.float32)
    low = jnp.dot(pick, mate_low_ref[...], preferred_element_type=jnp.float32)
    high = high.astype(jnp.bfloat16) + high_ref[...]
    low = low.astype(jnp.bfloat16) + low_ref[...]
    whole = high.astype(jnp.float32) + low.astype(jnp.float32)
    rows = whole.shape[0]
    both = jnp.concatenate([high, low], axis=0)
    cross = jnp.zeros((rows, refs[-1].shape[1]), jnp.float32)
    total = (1.0 / STRETCH**2) * jnp.sum(whole * whole, axis=1, keepdims=True)
    for part in range(PARTS):
        total = total + jnp.sum(refs[2 * part + 1][...], axis=0, keepdims=True)
    for part in range(PARTS):
        columns = refs[2 * part].shape[0] // 2
        piece = both[:, part * columns : (part + 1) * columns]
        product = jnp.dot(piece, refs[2 * part][:columns], preferred_element_type=jnp.float32)
        cross = cross + (product[:rows] + product[rows:])
        cross = cross + jnp.dot(piece[:rows], refs[2 * part][columns:], preferred_element_type=jnp.float32)
    total = jnp.maximum(total - (2.0 / STRETCH) * cross, 0.0)
    if send:
        total = jnp.where(total < SMALL, total * -RAISE_SMALL, total * RAISE)
    refs[-1][...] = total


def distances_of(pick, queries, vectors, send):
    return pl.pallas_call(
        lambda *refs: distance_kernel(send, *refs), out_shape=result((pick.shape[0], vectors[0].shape[1]), jnp.float32)
    )(*[in_vmem(array) for array in (pick, *queries, *vectors)])


def round_queries(queries):
    place = lax.broadcasted_iota(jnp.int32, queries.shape, 0) * queries.shape[1]
    place = (place + lax.broadcasted_iota(jnp.int32, queries.shape, 1)).astype(jnp.float32) * 0.618034
    offset = (place - jnp.floor(place)) * 2.0 - 1.0
    stretched = queries * STRETCH
    step = jnp.exp2(jnp.floor(jnp.log2(jnp.maximum(jnp.abs(stretched), 2.0**-14))) - 11.0)
    return (stretched + offset * step).astype(jnp.float16)


def split(rows):
    rows = rows.astype(jnp.float32)
    high = lax.reduce_precision(rows, 8, 7)
    return high.astype(jnp.bfloat16), (rows - high).astype(jnp.bfloat16)


def solution(mesh):
    blocks = mesh.shape["blk"]
    halves = mesh.shape["sub"]
    masks = []
    while (1 << len(masks)) < blocks:
        masks.append((blocks >> (len(masks) + 1)) | 1)

    def local(queries, centroids, code_ids, query_order):
        own_rows = queries.shape[0]
        mate = [(i, i ^ 1) for i in range(blocks)]
        code_ids = lax.ppermute(code_ids, "blk", mate)
        rows = round_queries(queries)
        for step, mask in enumerate(masks):
            arrived = lax.ppermute(rows, "blk", [(i, i ^ mask) for i in range(blocks)])
            if step + 1 < len(masks):
                rows = jnp.concatenate([rows, arrived], axis=0)
            else:
                own, late = split(rows), split(arrived)
        pick_mine, pick_theirs = make_picks(own_rows, masks, query_order.reshape(halves, -1))
        vectors = []
        for part in range(PARTS):
            vectors.extend(decode(part, code_ids, centroids))
        early = pick_early(pick_theirs, pick_mine, *own)
        theirs = distances_of(pick_theirs, (*early[:2], *late), vectors, True)
        across = [(i, (i ^ 1) ^ blocks) for i in range(halves * blocks)]
        arrived = lax.ppermute(theirs.astype(jnp.float16), ("sub", "blk"), across)
        mine = distances_of(pick_mine, (*early[2:], *late), vectors, False)
        mine = lax.ppermute(mine, "blk", mate)
        arrived = arrived.astype(jnp.float32)
        return mine + arrived * jnp.where(arrived < 0.0, -1.0 / RAISE_SMALL, 1.0 / RAISE)

    in_specs = (P("blk", "sub"), P("sub", None, None), P("sub", "blk"), P())
    return jax.shard_map(local, mesh=mesh, in_specs=in_specs, out_specs=P("sub", "blk"), check_vma=False)
```
